8 devices in a mesh: dp: 1 (over z), tp: 2 (over y), pp: 4 (over x, core).
Axes of the slice: x: 2, y: 2, z: 1, core: 2. Of those that a mesh axis runs over, the one named last changes fastest.
Arguments:
- tokens: int32 [4, 64], P('dp')
- labels: int32 [4, 64], P('dp')
- emb_table: bfloat16 [50272, 2048], P('tp')
- w_in: bfloat16 [4, 2048, 8192], P('pp', None, 'tp')
- w_out: bfloat16 [4, 8192, 2048], P('pp', 'tp')
Outputs:
- output 1: float32 [1], P('dp')
- output 2: float32 [4, 2048, 8192], P(('dp', 'pp'), None, 'tp')
- output 3: float32 [4, 8192, 2048], P(('dp', 'pp'), 'tp')
- output 4: float32 [50272, 2048], P(('dp', 'tp'))
All inputs are finite; a program needn't handle non-finite values.
Results may differ from the reference program's by a relative error of at most 0.0108034.
Values are sent between devices in bfloat16 or wider.
A program may use at most 1.75 GiB of HBM per device.

```python
import jax
import jax.numpy as jnp
from jax import lax

VOCAB_SIZE = 50272
MODEL_DIM = 2048
HIDDEN_DIM = 8192
NUM_STAGES = 4
MICRO_BATCHES = 4
SEQ_LEN = 64
NORM_EPS = 1e-6


def setup_inputs(seed: int = 0, part: int = 0) -> dict:
    part_key = jax.random.fold_in(jax.random.key(seed), part)
    key_outer, key_inner, key_rank, key_perm = jax.random.split(part_key, 4)
    id_shape = (MICRO_BATCHES, SEQ_LEN + 1)
    outer_cap = jax.random.randint(key_outer, id_shape, 1, VOCAB_SIZE + 1)
    inner_cap = jax.random.randint(key_inner, id_shape, 1, outer_cap + 1)
    rank_ids = jax.random.randint(key_rank, id_shape, 0, inner_cap)
    vocab_order = jax.random.permutation(key_perm, VOCAB_SIZE)
    id_seq = vocab_order[rank_ids].astype(jnp.int32)
    key_table, key_first, key_second = jax.random.split(jax.random.key(seed + 1), 3)
    emb_table = jax.random.normal(key_table, (VOCAB_SIZE, MODEL_DIM), jnp.float32) * MODEL_DIM ** -0.5
    w_in = jax.random.normal(key_first, (NUM_STAGES, MODEL_DIM, HIDDEN_DIM), jnp.float32) * MODEL_DIM ** -0.5
    w_out = jax.random.normal(key_second, (NUM_STAGES, HIDDEN_DIM, MODEL_DIM), jnp.float32) * (HIDDEN_DIM * NUM_STAGES / 2) ** -0.5
    return {'tokens': id_seq[:, :SEQ_LEN], 'labels': id_seq[:, 1:], 'emb_table': emb_table.astype(jnp.bfloat16), 'w_in': w_in.astype(jnp.bfloat16), 'w_out': w_out.astype(jnp.bfloat16)}


def reference(tokens, labels, emb_table, w_in, w_out):
    vocab_ids = jnp.arange(VOCAB_SIZE, dtype=jnp.int32)

    def layer_fwd(x_act, weights):
        w_one, w_two = weights
        hidden = jnp.dot(x_act, w_one, preferred_element_type=jnp.float32)
        gate_act = jax.nn.gelu(hidden).astype(jnp.bfloat16)
        branch_out = jnp.dot(gate_act, w_two, preferred_element_type=jnp.float32)
        return (x_act.astype(jnp.float32) + branch_out).astype(jnp.bfloat16), (x_act, hidden)

    def layer_bwd(grad_y, saved_act):
        x_act, hidden, w_one, w_two = saved_act
        gate_act, gelu_vjp = jax.vjp(jax.nn.gelu, hidden)
        grad_gate = jnp.dot(grad_y, w_two.T, preferred_element_type=jnp.float32)
        grad_hidden = gelu_vjp(grad_gate)[0].astype(jnp.bfloat16)
        grad_two = jnp.dot(gate_act.astype(jnp.bfloat16).T, grad_y, preferred_element_type=jnp.float32)
        grad_one = jnp.dot(x_act.T, grad_hidden, preferred_element_type=jnp.float32)
        grad_x = (grad_y.astype(jnp.float32) + jnp.dot(grad_hidden, w_one.T, preferred_element_type=jnp.float32)).astype(jnp.bfloat16)
        return grad_x, (grad_one, grad_two)

    def micro_step(carry_in, micro_in):
        loss_sum, acc_one, acc_two, acc_table = carry_in
        tok_row, lab_row = micro_in
        x_first = emb_table[tok_row]
        x_top, saved_fwd = lax.scan(layer_fwd, x_first, (w_in, w_out))
        x_wide = x_top.astype(jnp.float32)
        inv_rms = lax.rsqrt(jnp.mean(x_wide * x_wide, axis=-1, keepdims=True) + NORM_EPS)
        normed = x_wide * inv_rms
        normed_b = normed.astype(jnp.bfloat16)
        logits = jnp.dot(normed_b, emb_table.T, preferred_element_type=jnp.float32)
        log_norm = jax.nn.logsumexp(logits, axis=-1)
        target_hit = lab_row[:, None] == vocab_ids[None, :]
        target_logit = jnp.sum(jnp.where(target_hit, logits, 0.0), axis=-1)
        grad_logits = (jnp.exp(logits - log_norm[:, None]) - target_hit.astype(jnp.float32)).astype(jnp.bfloat16)
        head_grad = jnp.dot(grad_logits.T, normed_b, preferred_element_type=jnp.float32)
        grad_normed = jnp.dot(grad_logits, emb_table, preferred_element_type=jnp.float32)
        grad_top = (inv_rms * (grad_normed - normed * jnp.mean(normed * grad_normed, axis=-1, keepdims=True))).astype(jnp.bfloat16)
        grad_first, stage_grads = lax.scan(layer_bwd, grad_top, (saved_fwd[0], saved_fwd[1], w_in, w_out), reverse=True)
        new_table = (acc_table + head_grad).at[tok_row].add(grad_first.astype(jnp.float32))
        return (loss_sum + jnp.sum(log_norm - target_logit), acc_one + stage_grads[0], acc_two + stage_grads[1], new_table), None

    zero_state = (jnp.zeros((), jnp.float32), jnp.zeros((NUM_STAGES, MODEL_DIM, HIDDEN_DIM), jnp.float32), jnp.zeros((NUM_STAGES, HIDDEN_DIM, MODEL_DIM), jnp.float32), jnp.zeros((VOCAB_SIZE, MODEL_DIM), jnp.float32))
    totals = lax.scan(micro_step, zero_state, (tokens, labels))[0]
    mean_loss = (totals[0] / (MICRO_BATCHES * SEQ_LEN)).reshape(1)
    return mean_loss, totals[1], totals[2], totals[3]
```

```python
import jax
import jax.numpy as jnp
from jax import lax
from jax.sharding import PartitionSpec as P

NORM_EPS = 1e-6
AXES = ('tp', 'pp')


def contract(lhs, rhs, lhs_dim, rhs_dim):
    return lax.dot_general(lhs, rhs, (((lhs_dim,), (rhs_dim,)), ((), ())), preferred_element_type=jnp.float32)


def solution(mesh):
    pp_size = mesh.shape['pp']
    last = pp_size - 1

    def link(src_stage, dst_stage, cross):
        return [(t * pp_size + src_stage, (1 - t if cross else t) * pp_size + dst_stage) for t in range(2)]

    def send(value, src_stage, dst_stage, cross):
        return lax.ppermute(value, AXES, link(src_stage, dst_stage, cross))

    def device_fn(tokens, labels, emb_table, w_in, w_out):
        num_micro, seq_len = tokens.shape
        num_tok = num_micro * seq_len
        half = num_tok // 2
        vocab_rows, model_dim = emb_table.shape
        w_one = w_in[0]
        w_two = w_out[0]
        stage_idx = lax.axis_index('pp')
        tp_idx = lax.axis_index('tp')
        is_low = tp_idx == 0
        vocab_base = tp_idx * vocab_rows
        tok_local = tokens.reshape(num_tok) - vocab_base
        lab_local = labels.reshape(num_tok) - vocab_base
        row_ids = jnp.arange(vocab_rows, dtype=jnp.int32)

        def mine(value):
            return lax.dynamic_slice_in_dim(value, tp_idx * half, half, 0)

        def theirs(value):
            return lax.dynamic_slice_in_dim(value, (1 - tp_idx) * half, half, 0)

        def join(own, other):
            return jnp.concatenate([jnp.where(is_low, own, other), jnp.where(is_low, other, own)], axis=0)

        def reduce_half(partial, stage):
            return mine(partial) + send(theirs(partial), stage, stage, True)

        owned = (tok_local >= 0) & (tok_local < vocab_rows)
        looked_up = jnp.take(emb_table, jnp.clip(tok_local, 0, vocab_rows - 1), axis=0)
        looked_up = jnp.where(owned[:, None], looked_up, jnp.zeros_like(looked_up))
        x_act = looked_up + send(looked_up, 0, 0, True)

        for stage in range(pp_size):
            hidden = jnp.dot(x_act, w_one, preferred_element_type=jnp.float32)
            gate_act = jax.nn.gelu(hidden).astype(jnp.bfloat16)
            branch = reduce_half(jnp.dot(gate_act, w_two, preferred_element_type=jnp.float32), stage)
            y_half = (mine(x_act).astype(jnp.float32) + branch).astype(jnp.bfloat16)
            if stage < last:
                arrived = join(send(y_half, stage, stage + 1, False), send(y_half, stage, stage + 1, True))
                x_act = jnp.where(stage_idx == stage + 1, arrived, x_act)

        y_pair = join(y_half, send(y_half, last, last, True))
        y_mid = send(y_pair, last, 1, False)
        y_rest = send(y_pair, last, 2, False) + y_mid + send(y_mid, 1, 0, False)
        y_top = jnp.where(stage_idx == last, y_pair, y_rest)

        x_wide = y_top.astype(jnp.float32)
        inv_rms = lax.rsqrt(jnp.mean(x_wide * x_wide, axis=-1, keepdims=True) + NORM_EPS)
        normed = x_wide * inv_rms
        normed_b = normed.astype(jnp.bfloat16)
        logits = contract(emb_table, normed_b, 1, 1)
        target_hit = row_ids[:, None] == lab_local[None, :]
        local_max = jnp.max(logits, axis=0)
        local_sum = jnp.sum(jnp.exp(logits - local_max[None, :]), axis=0)
        local_target = jnp.sum(jnp.where(target_hit, logits, 0.0), axis=0)
        stats = jnp.stack([jnp.log(local_sum) + local_max, local_target])
        other = lax.ppermute(stats, 'tp', [(0, 1), (1, 0)])
        log_norm = jnp.logaddexp(stats[0], other[0])
        mean_loss = jnp.sum(log_norm - (stats[1] + other[1])) / num_tok
        grad_logits = (jnp.exp(logits - log_norm[None, :]) - target_hit.astype(jnp.float32)).astype(jnp.bfloat16)
        grad_normed = reduce_half(contract(grad_logits, emb_table, 0, 0), last)
        normed_h = mine(normed)
        grad_half = (mine(inv_rms) * (grad_normed - normed_h * jnp.mean(normed_h * grad_normed, axis=-1, keepdims=True))).astype(jnp.bfloat16)
        grad_y = join(grad_half, send(grad_half, last, last, True))

        gelu_vjp = jax.vjp(jax.nn.gelu, hidden)[1]
        for stage in range(last, -1, -1):
            grad_hidden = gelu_vjp(contract(grad_y, w_two, 1, 1))[0].astype(jnp.bfloat16)
            branch = reduce_half(contract(grad_hidden, w_one, 1, 1), stage)
            dx_half = (mine(grad_y).astype(jnp.float32) + branch).astype(jnp.bfloat16)
            if stage > 0:
                arrived = join(send(dx_half, stage, stage - 1, False), send(dx_half, stage, stage - 1, True))
                grad_y = jnp.where(stage_idx == stage - 1, arrived, grad_y)

        dx_pair = join(dx_half, send(dx_half, 0, 0, True))
        dx_mid = send(dx_pair, 0, 2, False)
        dx_rest = send(dx_pair, 0, 1, False) + dx_mid + send(dx_mid, 2, 3, False)
        dx_rows = jnp.where(stage_idx == 0, dx_pair, dx_rest)

        grad_two = contract(gate_act, grad_y, 0, 0)
        grad_one = contract(x_act, grad_hidden, 0, 0)
        token_hit = (row_ids[:, None] == tok_local[None, :]).astype(jnp.bfloat16)
        table_lhs = jnp.concatenate([grad_logits, token_hit], axis=1)
        grad_table = contract(table_lhs, jnp.concatenate([normed_b, dx_rows], axis=0), 1, 0)
        return mean_loss.reshape(1), grad_one[None], grad_two[None], grad_table

    return jax.shard_map(device_fn, mesh=mesh, in_specs=(P('dp', None), P('dp', None), P('tp', None), P('pp', None, 'tp'), P('pp', 'tp', None)), out_specs=(P('dp'), P(('dp', 'pp'), None, 'tp'), P(('dp', 'pp'), 'tp', None), P(('dp', 'tp'), None)), check_vma=False)
```

```python
import jax
import jax.numpy as jnp
from jax import lax
from jax.experimental import pallas as pl
from jax.experimental.pallas import tpu as pltpu
from jax.sharding import PartitionSpec as P

NORM_EPS = 1e-6
AXES = ('tp', 'pp')
NUM_CHUNKS = 2
ROW_GROUP = 8
TABLE_BLOCK = 528


def contract(lhs, rhs, lhs_dim, rhs_dim):
    return lax.dot_general(lhs, rhs, (((lhs_dim,), (rhs_dim,)), ((), ())), preferred_element_type=jnp.float32)


def empty_kernel(table_ref):
    pass


def head_kernel(base_ref, grad_ref, normed_ref, table_in, table_ref):
    table_ref[...] = jnp.dot(grad_ref[...], normed_ref[...], preferred_element_type=jnp.float32)


def head_rows(base, grad_logits, normed_b, table, num_steps):
    vocab_rows, model_dim = table.shape
    num_tok = normed_b.shape[0]
    return pl.pallas_call(
        head_kernel,
        out_shape=jax.ShapeDtypeStruct(table.shape, table.dtype),
        grid_spec=pltpu.PrefetchScalarGridSpec(
            num_scalar_prefetch=1,
            grid=(num_steps,),
            in_specs=[
                pl.BlockSpec((TABLE_BLOCK, num_tok), lambda i, base_ref: (base_ref[0] + i, 0)),
                pl.BlockSpec((num_tok, model_dim), lambda i, base_ref: (0, 0)),
                pl.BlockSpec(memory_space=pl.ANY),
            ],
            out_specs=pl.BlockSpec((TABLE_BLOCK, model_dim), lambda i, base_ref: (base_ref[0] + i, 0)),
        ),
        input_output_aliases={3: 0},
        compiler_params=pltpu.CompilerParams(dimension_semantics=('arbitrary',), vmem_limit_bytes=24 << 20),
        cost_estimate=pl.CostEstimate(flops=2 * num_steps * TABLE_BLOCK * model_dim * num_tok, bytes_accessed=4 * num_steps * TABLE_BLOCK * model_dim, transcendentals=0),
        name='head_rows',
    )(base, grad_logits, normed_b, table)


def add_kernel(group_ref, used_ref, pick_ref, rows_ref, table_in, table_ref, held_ref, sem):
    num_slots = group_ref.shape[0]
    part = 32 * ROW_GROUP

    def there(slot):
        return table_ref.at[pl.ds(pl.multiple_of(group_ref[slot] * ROW_GROUP, ROW_GROUP), ROW_GROUP), :]

    def here(slot):
        return held_ref.at[pl.ds(pl.multiple_of(slot * ROW_GROUP, ROW_GROUP), ROW_GROUP), :]

    def each(action):
        def step(slot, carry):
            @pl.when(used_ref[slot] == 1)
            def _():
                action(slot)
            return carry
        lax.fori_loop(0, num_slots, step, 0)

    each(lambda slot: pltpu.make_async_copy(there(slot), here(slot), sem.at[0]).start())
    each(lambda slot: pltpu.make_async_copy(there(slot), here(slot), sem.at[0]).wait())

    def add_part(index, carry):
        rows = pl.ds(pl.multiple_of(index * part, part), part)
        held_ref[rows, :] += jnp.dot(pick_ref[rows, :], rows_ref[...], preferred_element_type=jnp.float32)
        return carry

    lax.fori_loop(0, num_slots * ROW_GROUP // part, add_part, 0)
    each(lambda slot: pltpu.make_async_copy(here(slot), there(slot), sem.at[1]).start())
    each(lambda slot: pltpu.make_async_copy(here(slot), there(slot), sem.at[1]).wait())


def add_rows(group, used, pick, rows, table):
    num_slots, model_dim = rows.shape
    whole = pl.BlockSpec(memory_space=pltpu.VMEM)
    return pl.pallas_call(
        add_kernel,
        out_shape=jax.ShapeDtypeStruct(table.shape, table.dtype),
        in_specs=[pl.BlockSpec(memory_space=pltpu.SMEM), pl.BlockSpec(memory_space=pltpu.SMEM), whole, whole, pl.BlockSpec(memory_space=pl.ANY)],
        out_specs=pl.BlockSpec(memory_space=pl.ANY),
        scratch_shapes=[pltpu.VMEM((num_slots * ROW_GROUP, model_dim), jnp.float32), pltpu.SemaphoreType.DMA((2,))],
        input_output_aliases={4: 0},
        compiler_params=pltpu.CompilerParams(vmem_limit_bytes=32 << 20),
        name='add_rows',
    )(group, used, pick, rows, table)


def solution(mesh):
    pp_size = mesh.shape['pp']
    last = pp_size - 1

    def link(src_stage, dst_stage, cross):
        return [(t * pp_size + src_stage, (1 - t if cross else t) * pp_size + dst_stage) for t in range(2)]

    def send(value, src_stage, dst_stage, cross):
        return lax.ppermute(value, AXES, link(src_stage, dst_stage, cross))

    def device_fn(tokens, labels, emb_table, w_in, w_out):
        num_micro, seq_len = tokens.shape
        num_tok = num_micro * seq_len
        chunk_len = num_tok // NUM_CHUNKS
        half = chunk_len // 2
        chunks = range(NUM_CHUNKS)
        vocab_rows, model_dim = emb_table.shape
        w_one = w_in[0]
        w_two = w_out[0]
        stage_idx = lax.axis_index('pp')
        tp_idx = lax.axis_index('tp')
        is_low = tp_idx == 0
        vocab_base = tp_idx * vocab_rows
        tok_local = tokens.reshape(num_tok) - vocab_base
        lab_local = labels.reshape(num_tok) - vocab_base
        row_ids = jnp.arange(vocab_rows, dtype=jnp.int32)

        def cut(value, chunk):
            return value[chunk * chunk_len:(chunk + 1) * chunk_len]

        def mine(value):
            return lax.dynamic_slice_in_dim(value, tp_idx * half, half, 0)

        def theirs(value):
            return lax.dynamic_slice_in_dim(value, (1 - tp_idx) * half, half, 0)

        def join(own, other):
            return jnp.concatenate([jnp.where(is_low, own, other), jnp.where(is_low, other, own)], axis=0)

        def reduce_half(partial, stage):
            return mine(partial) + send(theirs(partial), stage, stage, True)

        def spread(value_half, source, far, near, rest):
            pair = join(value_half, send(value_half, source, source, True))
            middle = send(pair, source, far, False)
            others = send(pair, source, near, False) + middle + send(middle, far, rest, False)
            return jnp.where(stage_idx == source, pair, others)

        owned = (tok_local >= 0) & (tok_local < vocab_rows)
        looked_up = jnp.take(emb_table, jnp.clip(tok_local, 0, vocab_rows - 1), axis=0)
        looked_up = jnp.where(owned[:, None], looked_up, jnp.zeros_like(looked_up))
        x_act = [cut(looked_up, c) + send(cut(looked_up, c), 0, 0, True) for c in chunks]
        hidden, gate_act, y_half = [None] * NUM_CHUNKS, [None] * NUM_CHUNKS, [None] * NUM_CHUNKS

        for stage in range(pp_size):
            for c in chunks:
                hidden[c] = jnp.dot(x_act[c], w_one, preferred_element_type=jnp.float32)
                gate_act[c] = jax.nn.gelu(hidden[c]).astype(jnp.bfloat16)
                branch = reduce_half(jnp.dot(gate_act[c], w_two, preferred_element_type=jnp.float32), stage)
                y_half[c] = (mine(x_act[c]).astype(jnp.float32) + branch).astype(jnp.bfloat16)
                if stage < last:
                    arrived = join(send(y_half[c], stage, stage + 1, False), send(y_half[c], stage, stage + 1, True))
                    x_act[c] = jnp.where(stage_idx == stage + 1, arrived, x_act[c])

        y_top = jnp.concatenate([spread(y_half[c], last, 1, 2, 0) for c in chunks], axis=0)

        x_wide = y_top.astype(jnp.float32)
        inv_rms = lax.rsqrt(jnp.mean(x_wide * x_wide, axis=-1, keepdims=True) + NORM_EPS)
        normed = x_wide * inv_rms
        normed_b = normed.astype(jnp.bfloat16)
        logits = contract(emb_table, normed_b, 1, 1)
        target_hit = row_ids[:, None] == lab_local[None, :]
        local_max = jnp.max(logits, axis=0)
        local_sum = jnp.sum(jnp.exp(logits - local_max[None, :]), axis=0)
        local_target = jnp.sum(jnp.where(target_hit, logits, 0.0), axis=0)
        stats = jnp.stack([jnp.log(local_sum) + local_max, local_target])
        other = lax.ppermute(stats, 'tp', [(0, 1), (1, 0)])
        log_norm = jnp.logaddexp(stats[0], other[0])
        mean_loss = jnp.sum(log_norm - (stats[1] + other[1])) / num_tok
        grad_logits = (jnp.exp(logits - log_norm[None, :]) - target_hit.astype(jnp.float32)).astype(jnp.bfloat16)
        normed_part = contract(grad_logits, emb_table, 0, 0)
        grad_y = [None] * NUM_CHUNKS
        for c in chunks:
            grad_normed = reduce_half(cut(normed_part, c), last)
            normed_h = mine(cut(normed, c))
            grad_half = (mine(cut(inv_rms, c)) * (grad_normed - normed_h * jnp.mean(normed_h * grad_normed, axis=-1, keepdims=True))).astype(jnp.bfloat16)
            grad_y[c] = join(grad_half, send(grad_half, last, last, True))

        num_fill = (pp_size - 1) * NUM_CHUNKS
        fill_steps = pl.cdiv(pl.cdiv(vocab_rows, TABLE_BLOCK), num_fill)
        table = pl.pallas_call(empty_kernel, out_shape=jax.ShapeDtypeStruct((vocab_rows, model_dim), jnp.float32), out_specs=pl.BlockSpec(memory_space=pl.ANY), name='empty_table')()
        grad_hidden, dx_half = [jnp.zeros(hidden[0].shape, jnp.bfloat16)] * NUM_CHUNKS, [None] * NUM_CHUNKS
        for stage in range(last, -1, -1):
            for c in chunks:
                slot = (last - stage) * NUM_CHUNKS + c
                turn = slot - jnp.where(slot > (last - stage_idx) * NUM_CHUNKS, NUM_CHUNKS, 0)

                def run_stage(operands):
                    dy, wide, kept, held = operands
                    dh = jax.vjp(jax.nn.gelu, wide)[1](contract(dy, w_two, 1, 1))[0].astype(jnp.bfloat16)
                    return contract(dh, w_one, 1, 1), dh, held

                def fill_table(operands):
                    dy, wide, kept, held = operands
                    base = (turn * fill_steps).astype(jnp.int32).reshape(1)
                    return jnp.zeros(dy.shape, jnp.float32), kept, head_rows(base, grad_logits, normed_b, held, fill_steps)

                partial, grad_hidden[c], table = lax.cond(stage_idx == stage, run_stage, fill_table, (grad_y[c], hidden[c], grad_hidden[c], table))
                dx_half[c] = (mine(grad_y[c]).astype(jnp.float32) + reduce_half(partial, stage)).astype(jnp.bfloat16)
                if stage > 0:
                    arrived = join(send(dx_half[c], stage, stage - 1, False), send(dx_half[c], stage, stage - 1, True))
                    grad_y[c] = jnp.where(stage_idx == stage - 1, arrived, grad_y[c])

        dx_rows = jnp.concatenate([spread(dx_half[c], 0, 2, 1, 3) for c in chunks], axis=0)
        grad_two = contract(jnp.concatenate(gate_act, axis=0), jnp.concatenate(grad_y, axis=0), 0, 0)
        grad_one = contract(jnp.concatenate(x_act, axis=0), jnp.concatenate(grad_hidden, axis=0), 0, 0)
        slot_ids = jnp.arange(num_tok, dtype=jnp.int32)
        group = jnp.where(owned, tok_local // ROW_GROUP, -1)
        first = jnp.min(jnp.where(group[:, None] == group[None, :], slot_ids[None, :], num_tok), axis=1)
        used = (owned & (first == slot_ids)).astype(jnp.int32)
        slot_rows = (jnp.maximum(group, 0) * ROW_GROUP)[:, None] + jnp.arange(ROW_GROUP, dtype=jnp.int32)[None, :]
        pick = ((slot_rows[:, :, None] == tok_local[None, None, :]) & (used[:, None, None] == 1)).astype(jnp.bfloat16).reshape(num_tok * ROW_GROUP, num_tok)
        grad_table = add_rows(jnp.maximum(group, 0), used, pick, dx_rows, table)
        return mean_loss.reshape(1), grad_one[None], grad_two[None], grad_table

    return jax.shard_map(device_fn, mesh=mesh, in_specs=(P('dp', None), P('dp', None), P('tp', None), P('pp', None, 'tp'), P('pp', 'tp', None)), out_specs=(P('dp'), P(('dp', 'pp'), None, 'tp'), P(('dp', 'pp'), 'tp', None), P(('dp', 'tp'), None)), check_vma=False)
```

```python
import functools

import jax
import jax.numpy as jnp
from jax import lax
from jax.experimental import pallas as pl
from jax.experimental.pallas import tpu as pltpu
from jax.sharding import PartitionSpec as P

NORM_EPS = 1e-6
AXES = ('tp', 'pp')
NUM_CHUNKS = 1
HIDDEN_BLOCK = 512
ROW_GROUP = 8
TABLE_BLOCK = 528


def contract(lhs, rhs, lhs_dim, rhs_dim):
    return lax.dot_general(lhs, rhs, (((lhs_dim,), (rhs_dim,)), ((), ())), preferred_element_type=jnp.float32)


def empty_kernel(table_ref):
    pass


def head_kernel(base_ref, grad_ref, normed_ref, table_in, table_ref):
    table_ref[...] = jnp.dot(grad_ref[...], normed_ref[...], preferred_element_type=jnp.float32)


def head_rows(base, grad_logits, normed_b, table, num_steps):
    vocab_rows, model_dim = table.shape
    num_tok = normed_b.shape[0]
    return pl.pallas_call(
        head_kernel,
        out_shape=jax.ShapeDtypeStruct(table.shape, table.dtype),
        grid_spec=pltpu.PrefetchScalarGridSpec(
            num_scalar_prefetch=1,
            grid=(num_steps,),
            in_specs=[
                pl.BlockSpec((TABLE_BLOCK, num_tok), lambda i, base_ref: (base_ref[0] + i, 0)),
                pl.BlockSpec((num_tok, model_dim), lambda i, base_ref: (0, 0)),
                pl.BlockSpec(memory_space=pl.ANY),
            ],
            out_specs=pl.BlockSpec((TABLE_BLOCK, model_dim), lambda i, base_ref: (base_ref[0] + i, 0)),
        ),
        input_output_aliases={3: 0},
        compiler_params=pltpu.CompilerParams(dimension_semantics=('arbitrary',), vmem_limit_bytes=24 << 20),
        cost_estimate=pl.CostEstimate(flops=2 * num_steps * TABLE_BLOCK * model_dim * num_tok, bytes_accessed=4 * num_steps * TABLE_BLOCK * model_dim, transcendentals=0),
        name='head_rows',
    )(base, grad_logits, normed_b, table)


def add_kernel(group_ref, used_ref, pick_ref, rows_ref, table_in, table_ref, held_ref, sem):
    num_slots = group_ref.shape[0]
    part = 32 * ROW_GROUP

    def there(slot):
        return table_ref.at[pl.ds(pl.multiple_of(group_ref[slot] * ROW_GROUP, ROW_GROUP), ROW_GROUP), :]

    def here(slot):
        return held_ref.at[pl.ds(pl.multiple_of(slot * ROW_GROUP, ROW_GROUP), ROW_GROUP), :]

    def each(action):
        def step(slot, carry):
            @pl.when(used_ref[slot] == 1)
            def _():
                action(slot)
            return carry
        lax.fori_loop(0, num_slots, step, 0)

    each(lambda slot: pltpu.make_async_copy(there(slot), here(slot), sem.at[0]).start())
    each(lambda slot: pltpu.make_async_copy(there(slot), here(slot), sem.at[0]).wait())

    def add_part(index, carry):
        rows = pl.ds(pl.multiple_of(index * part, part), part)
        held_ref[rows, :] += jnp.dot(pick_ref[rows, :], rows_ref[...], preferred_element_type=jnp.float32)
        return carry

    lax.fori_loop(0, num_slots * ROW_GROUP // part, add_part, 0)
    each(lambda slot: pltpu.make_async_copy(here(slot), there(slot), sem.at[1]).start())
    each(lambda slot: pltpu.make_async_copy(here(slot), there(slot), sem.at[1]).wait())


def add_rows(group, used, pick, rows, table):
    num_slots, model_dim = rows.shape
    whole = pl.BlockSpec(memory_space=pltpu.VMEM)
    return pl.pallas_call(
        add_kernel,
        out_shape=jax.ShapeDtypeStruct(table.shape, table.dtype),
        in_specs=[pl.BlockSpec(memory_space=pltpu.SMEM), pl.BlockSpec(memory_space=pltpu.SMEM), whole, whole, pl.BlockSpec(memory_space=pl.ANY)],
        out_specs=pl.BlockSpec(memory_space=pl.ANY),
        scratch_shapes=[pltpu.VMEM((num_slots * ROW_GROUP, model_dim), jnp.float32), pltpu.SemaphoreType.DMA((2,))],
        input_output_aliases={4: 0},
        compiler_params=pltpu.CompilerParams(vmem_limit_bytes=32 << 20),
        name='add_rows',
    )(group, used, pick, rows, table)


def forward_kernel(x_ref, w_one_ref, w_two_ref, part_ref, *saved):
    hidden = jnp.dot(x_ref[...], w_one_ref[...], preferred_element_type=jnp.float32)
    gate_act = jax.nn.gelu(hidden).astype(jnp.bfloat16)
    update = jnp.dot(gate_act, w_two_ref[...], preferred_element_type=jnp.float32)

    @pl.when(pl.program_id(0) == 0)
    def _():
        part_ref[...] = update

    @pl.when(pl.program_id(0) > 0)
    def _():
        part_ref[...] += update

    if saved:
        saved[0][...] = hidden
        saved[1][...] = gate_act


def forward_stage(x_act, w_one, w_two, keep):
    rows, model_dim = x_act.shape
    hidden_cols = w_one.shape[1]
    columns = pl.BlockSpec((rows, HIDDEN_BLOCK), lambda j: (0, j))
    whole = pl.BlockSpec((rows, model_dim), lambda j: (0, 0))
    shapes = [jax.ShapeDtypeStruct((rows, model_dim), jnp.float32)]
    specs = [whole]
    if keep:
        shapes += [jax.ShapeDtypeStruct((rows, hidden_cols), jnp.float32), jax.ShapeDtypeStruct((rows, hidden_cols), jnp.bfloat16)]
        specs += [columns, columns]
    return pl.pallas_call(
        forward_kernel,
        out_shape=shapes,
        grid=(hidden_cols // HIDDEN_BLOCK,),
        in_specs=[whole, pl.BlockSpec((model_dim, HIDDEN_BLOCK), lambda j: (0, j)), pl.BlockSpec((HIDDEN_BLOCK, model_dim), lambda j: (j, 0))],
        out_specs=specs,
        compiler_params=pltpu.CompilerParams(dimension_semantics=('arbitrary',), vmem_limit_bytes=40 << 20),
        cost_estimate=pl.CostEstimate(flops=4 * rows * model_dim * hidden_cols, bytes_accessed=4 * model_dim * hidden_cols, transcendentals=rows * hidden_cols),
        name='forward_stage',
    )(x_act, w_one, w_two)


def backward_kernel(dy_ref, hidden_ref, w_one_ref, w_two_ref, part_ref, dh_ref):
    grad_gate = lax.dot_general(dy_ref[...], w_two_ref[...], (((1,), (1,)), ((), ())), preferred_element_type=jnp.float32)
    grad_hidden = jax.vjp(jax.nn.gelu, hidden_ref[...])[1](grad_gate)[0].astype(jnp.bfloat16)
    dh_ref[...] = grad_hidden
    update = lax.dot_general(grad_hidden, w_one_ref[...], (((1,), (1,)), ((), ())), preferred_element_type=jnp.float32)

    @pl.when(pl.program_id(0) == 0)
    def _():
        part_ref[...] = update

    @pl.when(pl.program_id(0) > 0)
    def _():
        part_ref[...] += update


def backward_stage(grad_y, hidden, w_one, w_two):
    rows, model_dim = grad_y.shape
    hidden_cols = w_one.shape[1]
    columns = pl.BlockSpec((rows, HIDDEN_BLOCK), lambda j: (0, j))
    whole = pl.BlockSpec((rows, model_dim), lambda j: (0, 0))
    return pl.pallas_call(
        backward_kernel,
        out_shape=[jax.ShapeDtypeStruct((rows, model_dim), jnp.float32), jax.ShapeDtypeStruct((rows, hidden_cols), jnp.bfloat16)],
        grid=(hidden_cols // HIDDEN_BLOCK,),
        in_specs=[whole, columns, pl.BlockSpec((model_dim, HIDDEN_BLOCK), lambda j: (0, j)), pl.BlockSpec((HIDDEN_BLOCK, model_dim), lambda j: (j, 0))],
        out_specs=[whole, columns],
        compiler_params=pltpu.CompilerParams(dimension_semantics=('arbitrary',), vmem_limit_bytes=40 << 20),
        cost_estimate=pl.CostEstimate(flops=4 * rows * model_dim * hidden_cols, bytes_accessed=4 * model_dim * hidden_cols, transcendentals=rows * hidden_cols),
        name='backward_stage',
    )(grad_y, hidden, w_one, w_two)


def logit_kernel(vocab_rows, emb_ref, normed_ref, label_ref, logit_ref, stat_ref, top_ref, sum_ref, hit_ref):
    step = pl.program_id(0)

    @pl.when(step == 0)
    def _():
        top_ref[...] = jnp.full(top_ref.shape, -jnp.inf, jnp.float32)
        sum_ref[...] = jnp.zeros(sum_ref.shape, jnp.float32)
        hit_ref[...] = jnp.zeros(hit_ref.shape, jnp.float32)

    logits = jnp.dot(emb_ref[...], normed_ref[...], preferred_element_type=jnp.float32)
    logit_ref[...] = logits
    row_ids = step * TABLE_BLOCK + lax.broadcasted_iota(jnp.int32, logits.shape, 0)
    inside = row_ids < vocab_rows
    logits = jnp.where(inside, logits, -jnp.inf)
    new_top = jnp.maximum(top_ref[...], jnp.max(logits, axis=0, keepdims=True))
    sum_ref[...] = sum_ref[...] * jnp.exp(top_ref[...] - new_top) + jnp.sum(jnp.exp(logits - new_top), axis=0, keepdims=True)
    hit_ref[...] += jnp.sum(jnp.where(inside & (row_ids == label_ref[...]), logits, 0.0), axis=0, keepdims=True)
    top_ref[...] = new_top

    @pl.when(step == pl.num_programs(0) - 1)
    def _():
        stat_ref[0:1, :] = top_ref[...] + jnp.log(sum_ref[...])
        stat_ref[1:2, :] = hit_ref[...]


def local_logits(emb_table, normed_b, lab_local):
    vocab_rows, model_dim = emb_table.shape
    num_tok = normed_b.shape[0]
    return pl.pallas_call(
        functools.partial(logit_kernel, vocab_rows),
        out_shape=[jax.ShapeDtypeStruct((vocab_rows, num_tok), jnp.float32), jax.ShapeDtypeStruct((2, num_tok), jnp.float32)],
        grid=(pl.cdiv(vocab_rows, TABLE_BLOCK),),
        in_specs=[pl.BlockSpec((TABLE_BLOCK, model_dim), lambda i: (i, 0)), pl.BlockSpec((model_dim, num_tok), lambda i: (0, 0)), pl.BlockSpec((1, num_tok), lambda i: (0, 0))],
        out_specs=[pl.BlockSpec((TABLE_BLOCK, num_tok), lambda i: (i, 0)), pl.BlockSpec((2, num_tok), lambda i: (0, 0))],
        scratch_shapes=[pltpu.VMEM((1, num_tok), jnp.float32)] * 3,
        compiler_params=pltpu.CompilerParams(dimension_semantics=('arbitrary',), vmem_limit_bytes=40 << 20),
        cost_estimate=pl.CostEstimate(flops=2 * vocab_rows * model_dim * num_tok, bytes_accessed=2 * vocab_rows * (model_dim + 2 * num_tok), transcendentals=vocab_rows * num_tok),
        name='local_logits',
    )(emb_table, normed_b.T, lab_local.reshape(1, num_tok))


def solution(mesh):
    pp_size = mesh.shape['pp']
    last = pp_size - 1

    def link(src_stage, dst_stage, cross):
        return [(t * pp_size + src_stage, (1 - t if cross else t) * pp_size + dst_stage) for t in range(2)]

    def send(value, src_stage, dst_stage, cross):
        return lax.ppermute(value, AXES, link(src_stage, dst_stage, cross))

    def device_fn(tokens, labels, emb_table, w_in, w_out):
        num_micro, seq_len = tokens.shape
        num_tok = num_micro * seq_len
        chunk_len = num_tok // NUM_CHUNKS
        half = chunk_len // 2
        chunks = range(NUM_CHUNKS)
        vocab_rows, model_dim = emb_table.shape
        w_one = w_in[0]
        w_two = w_out[0]
        stage_idx = lax.axis_index('pp')
        tp_idx = lax.axis_index('tp')
        is_low = tp_idx == 0
        vocab_base = tp_idx * vocab_rows
        tok_local = tokens.reshape(num_tok) - vocab_base
        lab_local = labels.reshape(num_tok) - vocab_base
        row_ids = jnp.arange(vocab_rows, dtype=jnp.int32)

        def cut(value, chunk):
            return value[chunk * chunk_len:(chunk + 1) * chunk_len]

        def mine(value):
            return lax.dynamic_slice_in_dim(value, tp_idx * half, half, 0)

        def theirs(value):
            return lax.dynamic_slice_in_dim(value, (1 - tp_idx) * half, half, 0)

        def join(own, other):
            return jnp.concatenate([jnp.where(is_low, own, other), jnp.where(is_low, other, own)], axis=0)

        def reduce_half(partial, stage):
            return mine(partial) + send(theirs(partial), stage, stage, True)

        def spread(value_half, source, far, near, rest):
            swapped = send(value_half, source, source, True)
            middle = send(value_half, source, far, False)
            own = send(value_half, source, near, False) + middle + send(middle, far, rest, False)
            pairs = [pair for stage in range(pp_size) if stage != source for pair in link(stage, stage, True)]
            other = lax.ppermute(own, AXES, pairs)
            return join(jnp.where(stage_idx == source, value_half, own), jnp.where(stage_idx == source, swapped, other))

        owned = (tok_local >= 0) & (tok_local < vocab_rows)
        looked_up = jnp.take(emb_table, jnp.clip(tok_local, 0, vocab_rows - 1), axis=0)
        looked_up = jnp.where(owned[:, None], looked_up, jnp.zeros_like(looked_up))
        x_act = [cut(looked_up, c) + send(cut(looked_up, c), 0, 0, True) for c in chunks]
        hidden, gate_act, y_half = [None] * NUM_CHUNKS, [None] * NUM_CHUNKS, [None] * NUM_CHUNKS

        for stage in range(pp_size):
            for c in chunks:
                partial, *saved = forward_stage(x_act[c], w_one, w_two, stage == last)
                if stage == last:
                    hidden[c], gate_act[c] = saved
                branch = reduce_half(partial, stage)
                y_half[c] = (mine(x_act[c]).astype(jnp.float32) + branch).astype(jnp.bfloat16)
                if stage < last:
                    arrived = join(send(y_half[c], stage, stage + 1, False), send(y_half[c], stage, stage + 1, True))
                    x_act[c] = jnp.where(stage_idx == stage + 1, arrived, x_act[c])

        y_top = jnp.concatenate([spread(y_half[c], last, 1, 2, 0) for c in chunks], axis=0)

        x_wide = y_top.astype(jnp.float32)
        inv_rms = lax.rsqrt(jnp.mean(x_wide * x_wide, axis=-1, keepdims=True) + NORM_EPS)
        normed = x_wide * inv_rms
        normed_b = normed.astype(jnp.bfloat16)
        logits, stats = local_logits(emb_table, normed_b, lab_local)
        target_hit = row_ids[:, None] == lab_local[None, :]
        other = lax.ppermute(stats, 'tp', [(0, 1), (1, 0)])
        log_norm = jnp.logaddexp(stats[0], other[0])
        mean_loss = jnp.sum(log_norm - (stats[1] + other[1])) / num_tok
        grad_logits = (jnp.exp(logits - log_norm[None, :]) - target_hit.astype(jnp.float32)).astype(jnp.bfloat16)
        normed_part = contract(grad_logits, emb_table, 0, 0)
        grad_y = [None] * NUM_CHUNKS
        for c in chunks:
            grad_normed = reduce_half(cut(normed_part, c), last)
            normed_h = mine(cut(normed, c))
            grad_half = (mine(cut(inv_rms, c)) * (grad_normed - normed_h * jnp.mean(normed_h * grad_normed, axis=-1, keepdims=True))).astype(jnp.bfloat16)
            grad_y[c] = join(grad_half, send(grad_half, last, last, True))

        num_fill = (pp_size - 1) * NUM_CHUNKS
        fill_steps = pl.cdiv(pl.cdiv(vocab_rows, TABLE_BLOCK), num_fill)
        table = pl.pallas_call(empty_kernel, out_shape=jax.ShapeDtypeStruct((vocab_rows, model_dim), jnp.float32), out_specs=pl.BlockSpec(memory_space=pl.ANY), name='empty_table')()
        grad_hidden, dx_half = [jnp.zeros(hidden[0].shape, jnp.bfloat16)] * NUM_CHUNKS, [None] * NUM_CHUNKS
        for stage in range(last, -1, -1):
            for c in chunks:
                slot = (last - stage) * NUM_CHUNKS + c
                turn = slot - jnp.where(slot > (last - stage_idx) * NUM_CHUNKS, NUM_CHUNKS, 0)

                def run_stage(operands):
                    dy, wide, kept, held = operands
                    part, dh = backward_stage(dy, wide, w_one, w_two)
                    return part, dh, held

                def fill_table(operands):
                    dy, wide, kept, held = operands
                    base = (turn * fill_steps).astype(jnp.int32).reshape(1)
                    return jnp.zeros(dy.shape, jnp.float32), kept, head_rows(base, grad_logits, normed_b, held, fill_steps)

                partial, grad_hidden[c], table = lax.cond(stage_idx == stage, run_stage, fill_table, (grad_y[c], hidden[c], grad_hidden[c], table))
                dx_half[c] = (mine(grad_y[c]).astype(jnp.float32) + reduce_half(partial, stage)).astype(jnp.bfloat16)
                if stage > 0:
                    arrived = join(send(dx_half[c], stage, stage - 1, False), send(dx_half[c], stage, stage - 1, True))
                    grad_y[c] = jnp.where(stage_idx == stage - 1, arrived, grad_y[c])

        dx_rows = jnp.concatenate([spread(dx_half[c], 0, 2, 1, 3) for c in chunks], axis=0)
        grad_two = contract(jnp.concatenate(gate_act, axis=0), jnp.concatenate(grad_y, axis=0), 0, 0)
        grad_one = contract(jnp.concatenate(x_act, axis=0), jnp.concatenate(grad_hidden, axis=0), 0, 0)
        slot_ids = jnp.arange(num_tok, dtype=jnp.int32)
        group = jnp.where(owned, tok_local // ROW_GROUP, -1)
        first = jnp.min(jnp.where(group[:, None] == group[None, :], slot_ids[None, :], num_tok), axis=1)
        used = (owned & (first == slot_ids)).astype(jnp.int32)
        slot_rows = (jnp.maximum(group, 0) * ROW_GROUP)[:, None] + jnp.arange(ROW_GROUP, dtype=jnp.int32)[None, :]
        pick = ((slot_rows[:, :, None] == tok_local[None, None, :]) & (used[:, None, None] == 1)).astype(jnp.bfloat16).reshape(num_tok * ROW_GROUP, num_tok)
        grad_table = add_rows(jnp.maximum(group, 0), used, pick, dx_rows, table)
        return mean_loss.reshape(1), grad_one[None], grad_two[None], grad_table

    return jax.shard_map(device_fn, mesh=mesh, in_specs=(P('dp', None), P('dp', None), P('tp', None), P('pp', None, 'tp'), P('pp', 'tp', None)), out_specs=(P('dp'), P(('dp', 'pp'), None, 'tp'), P(('dp', 'pp'), 'tp', None), P(('dp', 'tp'), None)), check_vma=False)
```

```python
import jax
import jax.numpy as jnp
from jax import lax
from jax.experimental import pallas as pl
from jax.experimental.pallas import tpu as pltpu
from jax.sharding import PartitionSpec as P

NORM_EPS = 1e-6
AXES = ('tp', 'pp')
NUM_CHUNKS = 1
HIDDEN_BLOCK = 512
ROW_GROUP = 8
TABLE_BLOCK = 528


def contract(lhs, rhs, lhs_dim, rhs_dim):
    return lax.dot_general(lhs, rhs, (((lhs_dim,), (rhs_dim,)), ((), ())), preferred_element_type=jnp.float32)


def empty_kernel(table_ref):
    pass


def head_kernel(base_ref, grad_ref, normed_ref, table_in, table_ref):
    table_ref[...] = jnp.dot(grad_ref[...], normed_ref[...], preferred_element_type=jnp.float32)


def head_rows(base, grad_logits, normed_b, table, num_steps):
    vocab_rows, model_dim = table.shape
    num_tok = normed_b.shape[0]
    return pl.pallas_call(
        head_kernel,
        out_shape=jax.ShapeDtypeStruct(table.shape, table.dtype),
        grid_spec=pltpu.PrefetchScalarGridSpec(
            num_scalar_prefetch=1,
            grid=(num_steps,),
            in_specs=[
                pl.BlockSpec((TABLE_BLOCK, num_tok), lambda i, base_ref: (base_ref[0] + i, 0)),
                pl.BlockSpec((num_tok, model_dim), lambda i, base_ref: (0, 0)),
                pl.BlockSpec(memory_space=pl.ANY),
            ],
            out_specs=pl.BlockSpec((TABLE_BLOCK, model_dim), lambda i, base_ref: (base_ref[0] + i, 0)),
        ),
        input_output_aliases={3: 0},
        compiler_params=pltpu.CompilerParams(dimension_semantics=('arbitrary',), vmem_limit_bytes=24 << 20),
        cost_estimate=pl.CostEstimate(flops=2 * num_steps * TABLE_BLOCK * model_dim * num_tok, bytes_accessed=4 * num_steps * TABLE_BLOCK * model_dim, transcendentals=0),
        name='head_rows',
    )(base, grad_logits, normed_b, table)


def add_kernel(group_ref, used_ref, pick_ref, rows_ref, table_in, table_ref, held_ref, sem):
    num_slots = group_ref.shape[0]
    part = 32 * ROW_GROUP

    def there(slot):
        return table_ref.at[pl.ds(pl.multiple_of(group_ref[slot] * ROW_GROUP, ROW_GROUP), ROW_GROUP), :]

    def here(slot):
        return held_ref.at[pl.ds(pl.multiple_of(slot * ROW_GROUP, ROW_GROUP), ROW_GROUP), :]

    def each(action):
        def step(slot, carry):
            @pl.when(used_ref[slot] == 1)
            def _():
                action(slot)
            return carry
        lax.fori_loop(0, num_slots, step, 0)

    each(lambda slot: pltpu.make_async_copy(there(slot), here(slot), sem.at[0]).start())
    each(lambda slot: pltpu.make_async_copy(there(slot), here(slot), sem.at[0]).wait())

    def add_part(index, carry):
        rows = pl.ds(pl.multiple_of(index * part, part), part)
        held_ref[rows, :] += jnp.dot(pick_ref[rows, :], rows_ref[...], preferred_element_type=jnp.float32)
        return carry

    lax.fori_loop(0, num_slots * ROW_GROUP // part, add_part, 0)
    each(lambda slot: pltpu.make_async_copy(here(slot), there(slot), sem.at[1]).start())
    each(lambda slot: pltpu.make_async_copy(here(slot), there(slot), sem.at[1]).wait())


def add_rows(group, used, pick, rows, table):
    num_slots, model_dim = rows.shape
    whole = pl.BlockSpec(memory_space=pltpu.VMEM)
    return pl.pallas_call(
        add_kernel,
        out_shape=jax.ShapeDtypeStruct(table.shape, table.dtype),
        in_specs=[pl.BlockSpec(memory_space=pltpu.SMEM), pl.BlockSpec(memory_space=pltpu.SMEM), whole, whole, pl.BlockSpec(memory_space=pl.ANY)],
        out_specs=pl.BlockSpec(memory_space=pl.ANY),
        scratch_shapes=[pltpu.VMEM((num_slots * ROW_GROUP, model_dim), jnp.float32), pltpu.SemaphoreType.DMA((2,))],
        input_output_aliases={4: 0},
        compiler_params=pltpu.CompilerParams(vmem_limit_bytes=32 << 20),
        name='add_rows',
    )(group, used, pick, rows, table)


def backward_kernel(dy_ref, hidden_ref, w_one_ref, w_two_ref, part_ref, dh_ref):
    grad_gate = lax.dot_general(dy_ref[...], w_two_ref[...], (((1,), (1,)), ((), ())), preferred_element_type=jnp.float32)
    grad_hidden = jax.vjp(jax.nn.gelu, hidden_ref[...])[1](grad_gate)[0].astype(jnp.bfloat16)
    dh_ref[...] = grad_hidden
    update = lax.dot_general(grad_hidden, w_one_ref[...], (((1,), (1,)), ((), ())), preferred_element_type=jnp.float32)

    @pl.when(pl.program_id(0) == 0)
    def _():
        part_ref[...] = update

    @pl.when(pl.program_id(0) > 0)
    def _():
        part_ref[...] += update


def backward_stage(grad_y, hidden, w_one, w_two):
    rows, model_dim = grad_y.shape
    hidden_cols = w_one.shape[1]
    columns = pl.BlockSpec((rows, HIDDEN_BLOCK), lambda j: (0, j))
    whole = pl.BlockSpec((rows, model_dim), lambda j: (0, 0))
    return pl.pallas_call(
        backward_kernel,
        out_shape=[jax.ShapeDtypeStruct((rows, model_dim), jnp.float32), jax.ShapeDtypeStruct((rows, hidden_cols), jnp.bfloat16)],
        grid=(hidden_cols // HIDDEN_BLOCK,),
        in_specs=[whole, columns, pl.BlockSpec((model_dim, HIDDEN_BLOCK), lambda j: (0, j)), pl.BlockSpec((HIDDEN_BLOCK, model_dim), lambda j: (j, 0))],
        out_specs=[whole, columns],
        compiler_params=pltpu.CompilerParams(dimension_semantics=('arbitrary',), vmem_limit_bytes=40 << 20),
        cost_estimate=pl.CostEstimate(flops=4 * rows * model_dim * hidden_cols, bytes_accessed=4 * model_dim * hidden_cols, transcendentals=rows * hidden_cols),
        name='backward_stage',
    )(grad_y, hidden, w_one, w_two)


def solution(mesh):
    pp_size = mesh.shape['pp']
    last = pp_size - 1

    def link(src_stage, dst_stage, cross):
        return [(t * pp_size + src_stage, (1 - t if cross else t) * pp_size + dst_stage) for t in range(2)]

    def send(value, src_stage, dst_stage, cross):
        return lax.ppermute(value, AXES, link(src_stage, dst_stage, cross))

    def device_fn(tokens, labels, emb_table, w_in, w_out):
        num_micro, seq_len = tokens.shape
        num_tok = num_micro * seq_len
        chunk_len = num_tok // NUM_CHUNKS
        half = chunk_len // 2
        chunks = range(NUM_CHUNKS)
        vocab_rows, model_dim = emb_table.shape
        w_one = w_in[0]
        w_two = w_out[0]
        stage_idx = lax.axis_index('pp')
        tp_idx = lax.axis_index('tp')
        is_low = tp_idx == 0
        vocab_base = tp_idx * vocab_rows
        tok_local = tokens.reshape(num_tok) - vocab_base
        lab_local = labels.reshape(num_tok) - vocab_base
        row_ids = jnp.arange(vocab_rows, dtype=jnp.int32)

        def cut(value, chunk):
            return value[chunk * chunk_len:(chunk + 1) * chunk_len]

        def mine(value):
            return lax.dynamic_slice_in_dim(value, tp_idx * half, half, 0)

        def theirs(value):
            return lax.dynamic_slice_in_dim(value, (1 - tp_idx) * half, half, 0)

        def join(own, other):
            return jnp.concatenate([jnp.where(is_low, own, other), jnp.where(is_low, other, own)], axis=0)

        def reduce_half(partial, stage):
            return mine(partial) + send(theirs(partial), stage, stage, True)

        def spread(value_half, source, far, near, rest):
            swapped = send(value_half, source, source, True)
            middle = send(value_half, source, far, False)
            own = send(value_half, source, near, False) + middle + send(middle, far, rest, False)
            pairs = [pair for stage in range(pp_size) if stage != source for pair in link(stage, stage, True)]
            other = lax.ppermute(own, AXES, pairs)
            return join(jnp.where(stage_idx == source, value_half, own), jnp.where(stage_idx == source, swapped, other))

        owned = (tok_local >= 0) & (tok_local < vocab_rows)
        looked_up = jnp.take(emb_table, jnp.clip(tok_local, 0, vocab_rows - 1), axis=0)
        looked_up = jnp.where(owned[:, None], looked_up, jnp.zeros_like(looked_up))
        x_act = [cut(looked_up, c) + send(cut(looked_up, c), 0, 0, True) for c in chunks]
        hidden, gate_act, y_half = [None] * NUM_CHUNKS, [None] * NUM_CHUNKS, [None] * NUM_CHUNKS

        for stage in range(pp_size):
            for c in chunks:
                hidden[c] = lax.optimization_barrier(jnp.dot(x_act[c], w_one, preferred_element_type=jnp.float32))
                gate_act[c] = jax.nn.gelu(hidden[c]).astype(jnp.bfloat16)
                branch = reduce_half(jnp.dot(gate_act[c], w_two, preferred_element_type=jnp.float32), stage)
                y_half[c] = (mine(x_act[c]).astype(jnp.float32) + branch).astype(jnp.bfloat16)
                if stage < last:
                    arrived = join(send(y_half[c], stage, stage + 1, False), send(y_half[c], stage, stage + 1, True))
                    x_act[c] = jnp.where(stage_idx == stage + 1, arrived, x_act[c])

        y_top = jnp.concatenate([spread(y_half[c], last, 1, 2, 0) for c in chunks], axis=0)

        x_wide = y_top.astype(jnp.float32)
        inv_rms = lax.rsqrt(jnp.mean(x_wide * x_wide, axis=-1, keepdims=True) + NORM_EPS)
        normed = x_wide * inv_rms
        normed_b = normed.astype(jnp.bfloat16)
        logits = contract(emb_table, normed_b, 1, 1)
        target_hit = row_ids[:, None] == lab_local[None, :]
        local_max = jnp.max(logits, axis=0)
        local_sum = jnp.sum(jnp.exp(logits - local_max[None, :]), axis=0)
        local_target = jnp.sum(jnp.where(target_hit, logits, 0.0), axis=0)
        stats = jnp.stack([jnp.log(local_sum) + local_max, local_target])
        other = lax.ppermute(stats, 'tp', [(0, 1), (1, 0)])
        log_norm = jnp.logaddexp(stats[0], other[0])
        mean_loss = jnp.sum(log_norm - (stats[1] + other[1])) / num_tok
        grad_logits = (jnp.exp(logits - log_norm[None, :]) - target_hit.astype(jnp.float32)).astype(jnp.bfloat16)
        normed_part = contract(grad_logits, emb_table, 0, 0)
        grad_y = [None] * NUM_CHUNKS
        for c in chunks:
            grad_normed = reduce_half(cut(normed_part, c), last)
            normed_h = mine(cut(normed, c))
            grad_half = (mine(cut(inv_rms, c)) * (grad_normed - normed_h * jnp.mean(normed_h * grad_normed, axis=-1, keepdims=True))).astype(jnp.bfloat16)
            grad_y[c] = join(grad_half, send(grad_half, last, last, True))

        num_fill = (pp_size - 1) * NUM_CHUNKS
        fill_steps = pl.cdiv(pl.cdiv(vocab_rows, TABLE_BLOCK), num_fill)
        table = pl.pallas_call(empty_kernel, out_shape=jax.ShapeDtypeStruct((vocab_rows, model_dim), jnp.float32), out_specs=pl.BlockSpec(memory_space=pl.ANY), name='empty_table')()
        grad_hidden, dx_half = [jnp.zeros(hidden[0].shape, jnp.bfloat16)] * NUM_CHUNKS, [None] * NUM_CHUNKS
        for stage in range(last, -1, -1):
            for c in chunks:
                slot = (last - stage) * NUM_CHUNKS + c
                turn = slot - jnp.where(slot > (last - stage_idx) * NUM_CHUNKS, NUM_CHUNKS, 0)

                def run_stage(operands):
                    dy, wide, kept, held = operands
                    part, dh = backward_stage(dy, wide, w_one, w_two)
                    return part, dh, held

                def fill_table(operands):
                    dy, wide, kept, held = operands
                    base = (turn * fill_steps).astype(jnp.int32).reshape(1)
                    return jnp.zeros(dy.shape, jnp.float32), kept, head_rows(base, grad_logits, normed_b, held, fill_steps)

                partial, grad_hidden[c], table = lax.cond(stage_idx == stage, run_stage, fill_table, (grad_y[c], hidden[c], grad_hidden[c], table))
                branch = reduce_half(partial, stage)
                if stage == 0:
                    grad_two = contract(gate_act[c], grad_y[c], 0, 0)
                    branch, grad_two = lax.optimization_barrier((branch, grad_two))
                dx_half[c] = (mine(grad_y[c]).astype(jnp.float32) + branch).astype(jnp.bfloat16)
                if stage > 0:
                    arrived = join(send(dx_half[c], stage, stage - 1, False), send(dx_half[c], stage, stage - 1, True))
                    grad_y[c] = jnp.where(stage_idx == stage - 1, arrived, grad_y[c])

        dx_rows = jnp.concatenate([spread(dx_half[c], 0, 2, 1, 3) for c in chunks], axis=0)
        grad_one = contract(jnp.concatenate(x_act, axis=0), jnp.concatenate(grad_hidden, axis=0), 0, 0)
        slot_ids = jnp.arange(num_tok, dtype=jnp.int32)
        group = jnp.where(owned, tok_local // ROW_GROUP, -1)
        first = jnp.min(jnp.where(group[:, None] == group[None, :], slot_ids[None, :], num_tok), axis=1)
        used = (owned & (first == slot_ids)).astype(jnp.int32)
        slot_rows = (jnp.maximum(group, 0) * ROW_GROUP)[:, None] + jnp.arange(ROW_GROUP, dtype=jnp.int32)[None, :]
        pick = ((slot_rows[:, :, None] == tok_local[None, None, :]) & (used[:, None, None] == 1)).astype(jnp.bfloat16).reshape(num_tok * ROW_GROUP, num_tok)
        grad_table = add_rows(jnp.maximum(group, 0), used, pick, dx_rows, table)
        return mean_loss.reshape(1), grad_one[None], grad_two[None], grad_table

    return jax.shard_map(device_fn, mesh=mesh, in_specs=(P('dp', None), P('dp', None), P('tp', None), P('pp', None, 'tp'), P('pp', 'tp', None)), out_specs=(P('dp'), P(('dp', 'pp'), None, 'tp'), P(('dp', 'pp'), 'tp', None), P(('dp', 'tp'), None)), check_vma=False)
```
